32 devices in a mesh: groups: 2 (over x), blk: 4 (over y, core), col: 4 (over z).
Axes of the slice: x: 2, y: 2, z: 4, core: 2. Of those that a mesh axis runs over, the one named last changes fastest.
Arguments:
- pair_block: bfloat16 [4096, 16384], P(('groups', 'blk'), 'col'), parts along dimension 0, may hold values from -1.5 to 1.5
- occ_energy: float32 [2], P('groups'), parts along dimension 0, may hold values from -1.5 to -0.3
- virt_energy: float32 [4096], P('groups'), parts along dimension 0, may hold values from 0.2 to 3
- frequency: float32 [2], P('groups'), parts along dimension 0, may hold values from 0.2 to 2
Outputs:
- dielectric: float32 [32768, 16384], P(('groups', 'col'), 'blk'), parts along dimension 0
The draws below stay inside these ranges and needn't reach their ends.
There are 2 independent parts, one for each index of `groups`. The reference program is written for one: setup_inputs(seed, part) draws one part's arguments, and reference() takes and returns one part's arrays. A program takes and returns all parts, laid end to end along the dimension named above; each array names one. Nothing has to cross between parts.
All inputs are finite; a program needn't handle non-finite values.
Results may differ from the reference program's by a relative error of at most 0.0027.
Values may be sent and summed in bfloat16 or wider, within the bound.
A program may use at most 192 MiB of HBM per device.

```python
import math
import jax
import jax.numpy as jnp
from jax import lax

NAUX = 16384
NVIRT = 2048
NOCC = 1
NPAIR = 2048


def block_scale(rng, extent, split, low, largest):
    def one(dim, shards_of):
        steps = jax.random.uniform(jax.random.fold_in(jax.random.fold_in(rng, 6), dim), (shards_of,), jnp.float32, low / len(split), largest / len(split))
        return jnp.repeat(jnp.exp(steps), extent[dim] // shards_of).reshape((-1,) + (1,) * (len(extent) - dim - 1))

    level = one(*split[0])
    for cut in split[1:]:
        level = level * one(*cut)
    return level


def gaussian(own_key, shape, scale, limit, shards=(), held_as=jnp.bfloat16):
    values = scale * jax.random.normal(own_key, shape, jnp.float32)
    if shards:
        values = values * block_scale(own_key, shape, shards, -0.22, 0.18)
    return jnp.clip(values, -limit, limit).astype(held_as)


def setup_inputs(seed: int = 0, part: int = 0) -> dict:
    streams_of = jax.random.split(jax.random.key(seed), 5)
    part_splits = jax.random.split(jax.random.fold_in(streams_of[4], part), 5)
    pair_block = gaussian(part_splits[0], (NPAIR, NAUX), (0.7 * NPAIR ** -0.25), 1.5, ((0, 4), (1, 4)))
    occ_energy = jnp.clip(jax.random.uniform(part_splits[1], (NOCC,), jnp.float32, -1.5, -0.3), -1.5, -0.3)
    virt_energy = jnp.clip(jnp.exp(jax.random.uniform(part_splits[2], (NVIRT,), jnp.float32, math.log(0.2), math.log(3.0))), 0.2, 3.0)
    frequency = jnp.clip(jnp.exp(jax.random.uniform(part_splits[3], (1,), jnp.float32, math.log(0.2), math.log(2.0))), 0.2, 2.0)
    return {"pair_block": pair_block, "occ_energy": occ_energy, "virt_energy": virt_energy, "frequency": frequency}


def reference(pair_block, occ_energy, virt_energy, frequency):
    gap = (virt_energy[None, :] - occ_energy[:, None]).reshape(-1)
    weights = 2.0 * gap / (gap * gap + frequency[0] * frequency[0])
    scaled = (pair_block.astype(jnp.float32) * weights[:, None]).astype(jnp.bfloat16)
    return lax.dot_general(scaled, pair_block, (((0,), (0,)), ((), ())), preferred_element_type=jnp.float32)
```

```python
import functools

import jax
import jax.numpy as jnp
from jax import lax
from jax.experimental import pallas as pl
from jax.experimental.pallas import tpu as pltpu
from jax.sharding import PartitionSpec as P

MESH = pl.DeviceIdType.MESH
CHUNKS = 16
UNITS = 8
TILES = 8
EARLY = 5
FIRST = 21
TICKS = 3 * CHUNKS + 4
TO_SIB, TO_OPP, UP, DOWN, FWD, DOWN_OPP, UP_OPP, UP_DIA, HOP_OWN, HOP_SIB, HOP_OPP, HOP_DIA, PASS, CROSS = range(14)
BOUNCE = 4


def pair_weights(occ_energy, virt_energy, frequency):
    gap = (virt_energy[None, :] - occ_energy[:, None]).reshape(-1)
    return 2.0 * gap / (gap * gap + frequency[0] * frequency[0])


def place():
    b, z = lax.axis_index("blk"), lax.axis_index("col")
    last = lax.axis_size("col") - 1
    y, k = b // 2, b % 2
    u, v = k + y - 2 * y * k, z + y * (last - 2 * z)
    return b, z, y, k, u, v


def when(cond, f):
    if cond is True:
        f()
    else:
        pl.when(cond)(f)


def load_columns(x, xz, xb, dst, sem, at_home, own, n, width):
    rows = x.shape[0]
    cols = pl.ds(pl.multiple_of(n * width, width), width)

    def piece(src, r):
        return pltpu.make_async_copy(src, dst.at[pl.ds(pl.multiple_of(r * rows, rows), rows)], sem.at[r])

    for r in range(4):
        band = pl.ds(r * rows, rows)

        @pl.when(jnp.logical_not(at_home))
        def _():
            piece(xb.at[band, cols], r).start()

        @pl.when(at_home & (own != r))
        def _():
            piece(xz.at[band, cols], r).start()

        @pl.when(at_home & (own == r))
        def _():
            piece(x.at[:, cols], r).start()


def await_columns(xb, dst, sem, rows, width):
    for r in range(4):
        band = pl.ds(r * rows, rows)
        pltpu.make_async_copy(xb.at[band, pl.ds(0, width)], dst.at[band], sem.at[r]).wait()


def gather_kernel(
    x, wt, xz, xb, tr, lhs_out, part,
    lhs, stage, rhs, acc, send, rz, rb, rt, stage_sem, rhs_sem, acc_sem, lhs_sem,
):
    rows, cols = x.shape
    step = cols // CHUNKS
    width = cols // UNITS
    tile = cols // TILES
    g = lax.axis_index("groups")
    b, z, y, k, u, v = place()
    dz = 1 - 2 * y
    own, sib, opp, dia = b, 2 * y + 1 - k, 2 * (1 - y) + k, 2 * (1 - y) + 1 - k
    lead0, lead1 = 3 * y, y + 1
    at_home = u == v

    def at(ref, r, c):
        return ref.at[
            pl.ds(pl.multiple_of(r * rows, rows), rows), pl.ds(pl.multiple_of(c * step, step), step)
        ]

    def copy(src, dst, ssem, rsem, dev):
        return pltpu.make_async_remote_copy(
            src_ref=src, dst_ref=dst, send_sem=ssem, recv_sem=rsem, device_id=(g, dev[0], dev[1]), device_id_type=MESH
        )

    to_sib, to_opp = (sib, z), (opp, z)
    up0, up1 = (lead0, z + dz), (lead1, z + dz)
    down1, down_same = (lead1, z - dz), (b, z - dz)
    across = (3 * (1 - y), z)

    def go(kind, c, src, ref, rsem, r, dev):
        copy(src, at(ref, r, c), send.at[kind, c], rsem.at[r, c], dev).start()

    def arrived(ref, rsem, r, c):
        copy(at(ref, r, c), at(ref, r, c), send.at[0, c], rsem.at[r, c], to_sib).wait_recv()

    hop0 = (u == 0) & ((v == 1) | (v == 2))
    hop1 = (u == 1) & (v == 2)
    lift = (v == 1) & (u == 1)

    barrier = pltpu.get_barrier_semaphore()
    for i in range(16):
        bb, zz = i // 4, i % 4

        @pl.when((bb != b) | (zz != z))
        def _():
            pl.semaphore_signal(barrier, inc=1, device_id=(g, bb, zz), device_id_type=MESH)

    pl.semaphore_wait(barrier, 15)

    def line_own(c):
        src = at(x, 0, c)
        pl.when(v == 1)(lambda: go(UP, c, src, xb, rb, own, up1))
        pl.when(v == 1)(lambda: go(DOWN, c, src, xb, rb, own, down1))

    line_own(0)
    line_own(1)

    @pl.loop(0, CHUNKS)
    def _(c):
        src = at(x, 0, c)
        go(TO_OPP, c, src, xz, rz, own, to_opp)
        pl.when(v == 0)(lambda: go(UP, c, src, xb, rb, own, up0))
        pl.when(v == 3)(lambda: go(DOWN, c, src, tr, rt, 0, down_same))
        go(TO_SIB, c, src, xz, rz, own, to_sib)

    def hop(kind, r, c, dev):
        arrived(xb, rb, r, c)
        go(kind, c, at(xb, r, c), xb, rb, r, dev)

    def end_waits(n):
        for i in range(CHUNKS // UNITS):
            c = n * (CHUNKS // UNITS) + i
            for r in (own, sib):
                pl.when(jnp.logical_not(at_home | hop0 | hop1))(lambda: arrived(xb, rb, r, c))
            for r in (opp, dia):
                pl.when(jnp.logical_not(at_home | hop1))(lambda: arrived(xb, rb, r, c))

    def stage_load(src):
        return pltpu.make_async_copy(src, stage, stage_sem.at[0])

    def band(ref, r):
        return ref.at[pl.ds(pl.multiple_of(r * rows, rows), rows)]

    def save(n, p, s):
        dst = part.at[pl.ds(pl.multiple_of(n * cols + p * tile, tile), tile)]
        return pltpu.make_async_copy(acc.at[s], dst, acc_sem.at[s])

    lhs_save = pltpu.make_async_copy(lhs, lhs_out, lhs_sem.at[0])

    @pl.loop(0, TICKS)
    def _(t):
        m, phase = t // 3, lax.rem(t, 3)

        @pl.when((t + 2 < CHUNKS) & (t >= 0))
        def _():
            line_own(t + 2)

        @pl.when(t < CHUNKS)
        def _():
            arrived(xz, rz, opp, t)
            src = at(xz, opp, t)
            pl.when(lift)(lambda: go(UP_OPP, t, src, xb, rb, opp, up1))
            pl.when(v == 1)(lambda: go(DOWN_OPP, t, src, xb, rb, opp, down1))
            go(FWD, t, src, xz, rz, opp, to_sib)

            @pl.when((u == 0) & (v == 1))
            def _():
                hop(HOP_OWN, own, t, up0)
                hop(HOP_SIB, sib, t, up0)

        @pl.when((t >= 1) & (t < CHUNKS + 1))
        def _():
            arrived(xz, rz, dia, t - 1)
            pl.when(lift)(lambda: go(UP_DIA, t - 1, at(xz, dia, t - 1), xb, rb, dia, up1))

        late = jnp.where(v == 0, m - 2, t - 2 + v)

        @pl.when((v <= 2) & ((v > 0) | (phase == 0)) & (late >= 0) & (late < CHUNKS))
        def _():
            arrived(tr, rt, 0, late)
            src = at(tr, 0, late)
            pl.when(v >= 1)(lambda: go(PASS, late, src, tr, rt, 0, down_same))
            go(CROSS, late, src, xb, rb, own, across)

        @pl.when(v == 2)
        def _():
            @pl.when(u == 1)
            def _():
                @pl.when(t == 0)
                def _():
                    hop(HOP_OWN, own, 0, up1)
                    hop(HOP_SIB, sib, 0, up1)

                @pl.when(((phase == 0) & (m >= 1) & (m + 1 < CHUNKS)))
                def _():
                    hop(HOP_OWN, own, m + 1, up1)

                @pl.when(t == 1)
                def _():
                    hop(HOP_OWN, own, 1, up1)

                @pl.when((phase == 1) & (m + 1 < CHUNKS))
                def _():
                    hop(HOP_SIB, sib, m + 1, up1)

                @pl.when((phase == 1) & (m < CHUNKS))
                def _():
                    hop(HOP_OPP, opp, m, up1)

                @pl.when((phase == 2) & (m >= 1) & (m <= CHUNKS))
                def _():
                    hop(HOP_DIA, dia, m - 1, up1)

            @pl.when(u == 0)
            def _():
                @pl.when((phase == 0) & (m >= 1) & (m <= CHUNKS))
                def _():
                    hop(HOP_SIB, sib, m - 1, up0)

                @pl.when((phase == 2) & (m < CHUNKS))
                def _():
                    hop(HOP_OWN, own, m, up0)

        @pl.when(t == 5)
        def _():
            @pl.loop(0, CHUNKS)
            def _(c):
                arrived(xz, rz, sib, c)

        fill = (t == 2) | (t == 6) | (t == CHUNKS + 1) | (t == CHUNKS + 2)

        @pl.when(fill)
        def _():
            r = jnp.where(t == 2, own, jnp.where(t == 6, sib, jnp.where(t == CHUNKS + 1, opp, dia)))
            stage_load(x).wait()
            scale = wt[:, pl.ds(pl.multiple_of(r * rows, rows), rows)]

            @pl.loop(0, TILES)
            def _(i):
                p = pl.ds(pl.multiple_of(i * tile, tile), tile)
                turned = stage[:, p].T.astype(jnp.float32) * scale
                lhs[p, pl.ds(pl.multiple_of(r * rows, rows), rows)] = turned.astype(jnp.bfloat16)

        pl.when(t == 1)(lambda: stage_load(x).start())
        pl.when(t == 5)(lambda: stage_load(band(xz, sib)).start())
        pl.when(t == CHUNKS)(lambda: stage_load(band(xz, opp)).start())
        pl.when(t == CHUNKS + 1)(lambda: stage_load(band(xz, dia)).start())
        pl.when(t == CHUNKS + 2)(lambda: lhs_save.start())

        work = t - FIRST
        n, q = work // 4, lax.rem(work, 4)

        @pl.when((work >= 0) & (work < 4 * EARLY))
        def _():
            s = lax.rem(n, 2)

            @pl.when(q == 0)
            def _():
                await_columns(xb, rhs.at[s], rhs_sem.at[s], rows, width)

            for j in range(2):
                p = 2 * q + j
                pl.when(work >= 1)(lambda: save(0, 0, j).wait())
                acc[j] = jnp.dot(
                    lhs[pl.ds(pl.multiple_of(p * tile, tile), tile), :], rhs[s], preferred_element_type=jnp.float32
                )
                save(n, p, j).start()

        ahead = work + 1
        n_ahead = ahead // 4

        @pl.when((ahead >= 0) & (ahead < 4 * EARLY) & (lax.rem(ahead, 4) == 0))
        def _():
            end_waits(n_ahead)
            s = lax.rem(n_ahead, 2)
            load_columns(x, xz, xb, rhs.at[s], rhs_sem.at[s], at_home, own, n_ahead, width)

    for j in range(2):
        save(0, 0, j).wait()
    lhs_save.wait()

    @pl.loop(EARLY, UNITS)
    def _(n):
        end_waits(n)

    sends = [
        (TO_SIB, True), (TO_OPP, True), (FWD, True),
        (UP, v <= 1), (DOWN, (v == 1) | (v == 3)), (DOWN_OPP, v == 1),
        (UP_OPP, lift), (UP_DIA, lift),
        (HOP_OWN, hop0 | hop1), (HOP_SIB, hop0 | hop1), (HOP_OPP, hop1), (HOP_DIA, hop1),
        (PASS, (v == 1) | (v == 2)), (CROSS, v <= 2),
    ]

    @pl.loop(0, CHUNKS)
    def _(c):
        for kind, cond in sends:
            when(cond, lambda: copy(at(x, 0, c), at(xz, 0, c), send.at[kind, c], rz.at[0, c], to_sib).wait_send())


def gather(pair_block, weights):
    rows, cols = pair_block.shape
    width, tile = cols // UNITS, cols // TILES
    bf16, f32 = jnp.bfloat16, jnp.float32
    full = jax.ShapeDtypeStruct((4 * rows, cols), bf16)
    return pl.pallas_call(
        gather_kernel,
        out_shape=(
            full,
            full,
            jax.ShapeDtypeStruct((rows, cols), bf16),
            jax.ShapeDtypeStruct((cols, 4 * rows), bf16),
            jax.ShapeDtypeStruct((EARLY * cols, width), f32),
        ),
        in_specs=[pl.BlockSpec(memory_space=pl.ANY), pl.BlockSpec(memory_space=pltpu.VMEM)],
        out_specs=[pl.BlockSpec(memory_space=pl.ANY)] * 5,
        scratch_shapes=[
            pltpu.VMEM((cols, 4 * rows), bf16),
            pltpu.VMEM((rows, cols), bf16),
            pltpu.VMEM((2, 4 * rows, width), bf16),
            pltpu.VMEM((2, tile, width), f32),
            pltpu.SemaphoreType.DMA((14, CHUNKS)),
            pltpu.SemaphoreType.DMA((4, CHUNKS)),
            pltpu.SemaphoreType.DMA((4, CHUNKS)),
            pltpu.SemaphoreType.DMA((1, CHUNKS)),
            pltpu.SemaphoreType.DMA((1,)),
            pltpu.SemaphoreType.DMA((2, 4)),
            pltpu.SemaphoreType.DMA((2,)),
            pltpu.SemaphoreType.DMA((1,)),
        ],
        compiler_params=pltpu.CompilerParams(collective_id=0, has_side_effects=True),
    )(pair_block, weights[None, :])


def finish_kernel(
    x, xz, xb, lhs_in, part, out,
    lhs, rhs, acc, hold, lhs_sem, rhs_sem, acc_sem, in_sem, out_sem,
):
    rows, cols = x.shape
    width, tile = cols // UNITS, cols // TILES
    late = UNITS - EARLY
    moves = EARLY * TILES // 2
    b, z, y, k, u, v = place()

    def span(i, size):
        return pl.ds(pl.multiple_of(i * size, size), size)

    def take(i):
        s = lax.rem(i, BOUNCE)
        return pltpu.make_async_copy(part.at[span(i, 2 * tile)], hold.at[s], in_sem.at[s])

    def put(i):
        s = lax.rem(i, BOUNCE)
        n, p = i // (TILES // 2), lax.rem(i, TILES // 2)
        return pltpu.make_async_copy(hold.at[s], out.at[span(p, 2 * tile), span(n, width)], out_sem.at[s])

    def fetch(p):
        s = lax.rem(p, 2)
        return pltpu.make_async_copy(lhs_in.at[span(p, tile)], lhs.at[s], lhs_sem.at[s])

    def store(p, n):
        return pltpu.make_async_copy(acc.at[n], out.at[span(p, tile), span(EARLY + n, width)], acc_sem.at[n])

    fetch(0).start()
    for n in range(late):
        load_columns(x, xz, xb, rhs.at[n], rhs_sem.at[n], u == v, b, EARLY + n, width)
    for i in range(2):
        take(i).start()
    fetch(1).start()

    def shift(i):
        @pl.when(i < moves)
        def _():
            take(i).wait()
            put(i).start()

        @pl.when(i + 2 < moves)
        def _():
            pl.when(i + 2 >= BOUNCE)(lambda: put(i + 2 - BOUNCE).wait())
            take(i + 2).start()

    @pl.loop(0, TILES)
    def _(p):
        fetch(p).wait()
        for n in range(late):
            pl.when(p == 0)(lambda: await_columns(xb, rhs.at[n], rhs_sem.at[n], rows, width))
            pl.when(p >= 1)(lambda: store(p - 1, n).wait())
            acc[n] = jnp.dot(lhs[lax.rem(p, 2)], rhs[n], preferred_element_type=jnp.float32)
            store(p, n).start()
            shift(p * late + n)

        pl.when(p + 2 < TILES)(lambda: fetch(p + 2).start())

    for i in range(TILES * late, moves):
        shift(i)
    for n in range(late):
        store(TILES - 1, n).wait()
    for i in range(max(0, moves - BOUNCE), moves):
        put(i).wait()


def finish(pair_block, xz, xb, lhs, part):
    rows, cols = pair_block.shape
    width, tile = cols // UNITS, cols // TILES
    late = UNITS - EARLY
    bf16, f32 = jnp.bfloat16, jnp.float32
    return pl.pallas_call(
        finish_kernel,
        out_shape=jax.ShapeDtypeStruct((cols, cols), f32),
        in_specs=[pl.BlockSpec(memory_space=pl.ANY)] * 5,
        out_specs=pl.BlockSpec(memory_space=pl.ANY),
        scratch_shapes=[
            pltpu.VMEM((2, tile, 4 * rows), bf16),
            pltpu.VMEM((late, 4 * rows, width), bf16),
            pltpu.VMEM((late, tile, width), f32),
            pltpu.VMEM((BOUNCE, 2 * tile, width), f32),
            pltpu.SemaphoreType.DMA((2,)),
            pltpu.SemaphoreType.DMA((late, 4)),
            pltpu.SemaphoreType.DMA((late,)),
            pltpu.SemaphoreType.DMA((BOUNCE,)),
            pltpu.SemaphoreType.DMA((BOUNCE,)),
        ],
    )(pair_block, xz, xb, lhs, part)


def shards(square, pair_block, occ_energy, virt_energy, frequency):
    weights = pair_weights(occ_energy, virt_energy, frequency)
    if square:
        xz, xb, _, lhs, part = gather(pair_block, weights)
        return finish(pair_block, xz, xb, lhs, part)
    row_full = lax.all_gather(pair_block, "col", axis=1, tiled=True)
    column_slab = lax.all_to_all(row_full, "blk", split_axis=1, concat_axis=0, tiled=True)
    own_columns = lax.all_gather(pair_block, "blk", axis=0, tiled=True)
    scaled = (own_columns.astype(jnp.float32) * weights[:, None]).astype(jnp.bfloat16)
    return lax.dot_general(
        scaled, column_slab, (((0,), (0,)), ((), ())), preferred_element_type=jnp.float32
    )


def solution(mesh):
    square = mesh.shape["blk"] == 4 and mesh.shape["col"] == 4
    return jax.shard_map(
        functools.partial(shards, square),
        mesh=mesh,
        in_specs=(P(("groups", "blk"), "col"), P("groups"), P("groups"), P("groups")),
        out_specs=P(("groups", "col"), "blk"),
        check_vma=False,
    )
```

```python
import functools

import jax
import jax.numpy as jnp
from jax import lax
from jax.experimental import pallas as pl
from jax.experimental.pallas import tpu as pltpu
from jax.sharding import PartitionSpec as P

MESH = pl.DeviceIdType.MESH
CHUNKS = 32
UNITS = 8
TILES = 8
EARLY = 7
FIRST = CHUNKS + 11
HELD = 3 * CHUNKS // 4
TICKS = 3 * CHUNKS + 4
PER_TICK = 32 // CHUNKS
SPAN = TILES // PER_TICK
MIB = 1 << 20
TO_SIB, TO_OPP, UP, DOWN, FWD, DOWN_OPP, UP_OPP, UP_DIA, HOP_OWN, HOP_SIB, HOP_OPP, HOP_DIA, PASS, CROSS = range(14)
SLOTS = 6
STRIPS = 4


def pair_weights(occ_energy, virt_energy, frequency):
    gap = (virt_energy[None, :] - occ_energy[:, None]).reshape(-1)
    return 2.0 * gap / (gap * gap + frequency[0] * frequency[0])


def place():
    b, z = lax.axis_index("blk"), lax.axis_index("col")
    last = lax.axis_size("col") - 1
    y, k = b // 2, b % 2
    u, v = k + y - 2 * y * k, z + y * (last - 2 * z)
    return b, z, y, k, u, v


def when(cond, f):
    if cond is True:
        f()
    else:
        pl.when(cond)(f)


def load_columns(x, xz, xb, dst, sem, at_home, own, n, width):
    rows = x.shape[0]
    cols = pl.ds(pl.multiple_of(n * width, width), width)

    def piece(src, r):
        return pltpu.make_async_copy(src, dst.at[pl.ds(pl.multiple_of(r * rows, rows), rows)], sem.at[r])

    for r in range(4):
        band = pl.ds(r * rows, rows)

        @pl.when(jnp.logical_not(at_home))
        def _():
            piece(xb.at[band, cols], r).start()

        @pl.when(at_home & (own != r))
        def _():
            piece(xz.at[band, cols], r).start()

        @pl.when(at_home & (own == r))
        def _():
            piece(x.at[:, cols], r).start()


def await_columns(xb, dst, sem, rows, width):
    for r in range(4):
        band = pl.ds(r * rows, rows)
        pltpu.make_async_copy(xb.at[band, pl.ds(0, width)], dst.at[band], sem.at[r]).wait()


def gather_kernel(
    x, wt, xz, xb, tr, lhs, kept,
    stage, rhs, send, rz, rb, rt, stage_sem, rhs_sem,
):
    rows, cols = x.shape
    step = cols // CHUNKS
    width = cols // UNITS
    tile = cols // TILES
    g = lax.axis_index("groups")
    b, z, y, k, u, v = place()
    dz = 1 - 2 * y
    own, sib, opp, dia = b, 2 * y + 1 - k, 2 * (1 - y) + k, 2 * (1 - y) + 1 - k
    lead0, lead1 = 3 * y, y + 1
    at_home = u == v

    def at(ref, r, c):
        return ref.at[
            pl.ds(pl.multiple_of(r * rows, rows), rows), pl.ds(pl.multiple_of(c * step, step), step)
        ]

    def copy(src, dst, ssem, rsem, dev):
        return pltpu.make_async_remote_copy(
            src_ref=src, dst_ref=dst, send_sem=ssem, recv_sem=rsem, device_id=(g, dev[0], dev[1]), device_id_type=MESH
        )

    to_sib, to_opp = (sib, z), (opp, z)
    up0, up1 = (lead0, z + dz), (lead1, z + dz)
    down1, down_same = (lead1, z - dz), (b, z - dz)
    across = (3 * (1 - y), z)

    def go(kind, c, src, ref, rsem, r, dev):
        copy(src, at(ref, r, c), send.at[kind, c], rsem.at[r, c], dev).start()

    def arrived(ref, rsem, r, c):
        copy(at(ref, r, c), at(ref, r, c), send.at[0, c], rsem.at[r, c], to_sib).wait_recv()

    hop0 = (u == 0) & ((v == 1) | (v == 2))
    hop1 = (u == 1) & (v == 2)
    lift = (v == 1) & (u == 1)

    barrier = pltpu.get_barrier_semaphore()
    for i in range(16):
        bb, zz = i // 4, i % 4

        @pl.when((bb != b) | (zz != z))
        def _():
            pl.semaphore_signal(barrier, inc=1, device_id=(g, bb, zz), device_id_type=MESH)

    pl.semaphore_wait(barrier, 15)

    def line_own(c):
        src = at(x, 0, c)
        pl.when(v == 1)(lambda: go(UP, c, src, xb, rb, own, up1))
        pl.when((v == 1) & (c < HELD))(lambda: go(DOWN, c, src, xb, rb, own, down1))

    line_own(0)
    line_own(1)

    @pl.loop(0, CHUNKS)
    def _(c):
        src = at(x, 0, c)
        go(TO_OPP, c, src, xz, rz, own, to_opp)
        pl.when(v == 0)(lambda: go(UP, c, src, xb, rb, own, up0))
        pl.when(v == 3)(lambda: go(DOWN, c, src, tr, rt, 0, down_same))
        go(TO_SIB, c, src, xz, rz, own, to_sib)

    def hop(kind, r, c, dev):
        arrived(xb, rb, r, c)
        go(kind, c, at(xb, r, c), xb, rb, r, dev)

    def end_waits(n):
        for i in range(CHUNKS // UNITS):
            c = n * (CHUNKS // UNITS) + i
            for r in (own, sib):
                pl.when(jnp.logical_not(at_home | hop0 | hop1))(lambda: arrived(xb, rb, r, c))
            for r in (opp, dia):
                pl.when(jnp.logical_not(at_home | hop1))(lambda: arrived(xb, rb, r, c))

    def stage_load(src):
        return pltpu.make_async_copy(src, stage, stage_sem.at[0])

    def band(ref, r):
        return ref.at[pl.ds(pl.multiple_of(r * rows, rows), rows)]

    @pl.loop(0, TICKS)
    def _(t):
        m, phase = t // 3, lax.rem(t, 3)

        @pl.when((t + 2 < CHUNKS) & (t >= 0))
        def _():
            line_own(t + 2)

        @pl.when(t < CHUNKS)
        def _():
            arrived(xz, rz, opp, t)
            src = at(xz, opp, t)
            pl.when(lift)(lambda: go(UP_OPP, t, src, xb, rb, opp, up1))
            pl.when((v == 1) & (t < HELD))(lambda: go(DOWN_OPP, t, src, xb, rb, opp, down1))
            go(FWD, t, src, xz, rz, opp, to_sib)

            @pl.when((u == 0) & (v == 1))
            def _():
                hop(HOP_OWN, own, t, up0)
                hop(HOP_SIB, sib, t, up0)

        @pl.when((t >= 1) & (t < CHUNKS + 1))
        def _():
            arrived(xz, rz, dia, t - 1)
            pl.when(lift)(lambda: go(UP_DIA, t - 1, at(xz, dia, t - 1), xb, rb, dia, up1))

        held = HELD + t - (CHUNKS + 2)

        @pl.when((v == 1) & (held >= HELD) & (held < CHUNKS))
        def _():
            go(DOWN, held, at(x, 0, held), xb, rb, own, down1)
            go(DOWN_OPP, held, at(xz, opp, held), xb, rb, opp, down1)

        slow, burst = m - 2, t - 2 * HELD
        late = jnp.where(v == 0, jnp.where(burst >= HELD - 3, burst, slow), t - 2 + v)
        paced = (v > 0) | ((phase == 1) & (slow < HELD - 3)) | (burst >= HELD - 3)

        @pl.when((v <= 2) & paced & (late >= 0) & (late < CHUNKS))
        def _():
            arrived(tr, rt, 0, late)
            src = at(tr, 0, late)
            pl.when(v >= 1)(lambda: go(PASS, late, src, tr, rt, 0, down_same))
            go(CROSS, late, src, xb, rb, own, across)

        @pl.when(hop1)
        def _():
            @pl.when((phase == 0) & (m >= 2) & (m < CHUNKS + 2))
            def _():
                hop(HOP_DIA, dia, m - 2, up1)

            @pl.when(t < 2)
            def _():
                hop(HOP_OWN, own, t, up1)
                hop(HOP_SIB, sib, t, up1)

            @pl.when((phase == 1) & (m < CHUNKS - 2))
            def _():
                hop(HOP_OWN, own, m + 2, up1)

            @pl.when((phase == 2) & (m < CHUNKS - 2))
            def _():
                hop(HOP_SIB, sib, m + 2, up1)

            @pl.when((phase == 2) & (m < CHUNKS))
            def _():
                hop(HOP_OPP, opp, m, up1)

        @pl.when((u == 0) & (v == 2) & (m >= 1) & (m <= CHUNKS))
        def _():
            pl.when(phase == 0)(lambda: hop(HOP_OWN, own, m - 1, up0))
            pl.when(phase == 1)(lambda: hop(HOP_SIB, sib, m - 1, up0))

        @pl.when(t == 9)
        def _():
            @pl.loop(0, CHUNKS)
            def _(c):
                arrived(xz, rz, sib, c)

        fill = (t == 3) | (t == 10) | (t == CHUNKS + 1) | (t == CHUNKS + 2)

        @pl.when(fill)
        def _():
            r = jnp.where(t == 3, own, jnp.where(t == 10, sib, jnp.where(t == CHUNKS + 1, opp, dia)))
            stage_load(x).wait()
            scale = wt[:, pl.ds(pl.multiple_of(r * rows, rows), rows)]

            @pl.loop(0, TILES)
            def _(i):
                p = pl.ds(pl.multiple_of(i * tile, tile), tile)
                turned = stage[:, p].T.astype(jnp.float32) * scale
                lhs[p, pl.ds(pl.multiple_of(r * rows, rows), rows)] = turned.astype(jnp.bfloat16)

        pl.when(t == 1)(lambda: stage_load(x).start())
        pl.when(t == 9)(lambda: stage_load(band(xz, sib)).start())
        pl.when(t == CHUNKS)(lambda: stage_load(band(xz, opp)).start())
        pl.when(t == CHUNKS + 1)(lambda: stage_load(band(xz, dia)).start())

        work = t - FIRST
        n, q = work // SPAN, lax.rem(work, SPAN)

        @pl.when((work >= 0) & (work < SPAN * EARLY))
        def _():
            s = lax.rem(n, 2)

            @pl.when(q == 0)
            def _():
                await_columns(xb, rhs.at[s], rhs_sem.at[s], rows, width)

            for j in range(PER_TICK):
                p = PER_TICK * q + j
                got = jnp.dot(
                    lhs[pl.ds(pl.multiple_of(p * tile, tile), tile), :], rhs[s], preferred_element_type=jnp.float32
                )
                kept[
                    pl.ds(pl.multiple_of(p * tile, tile), tile), pl.ds(pl.multiple_of(n * width, width), width)
                ] = got.astype(jnp.bfloat16)

        ahead = work + 1
        n_ahead = ahead // SPAN

        @pl.when((ahead >= 0) & (ahead < SPAN * EARLY) & (lax.rem(ahead, SPAN) == 0))
        def _():
            end_waits(n_ahead)
            s = lax.rem(n_ahead, 2)
            load_columns(x, xz, xb, rhs.at[s], rhs_sem.at[s], at_home, own, n_ahead, width)

    @pl.loop(EARLY, UNITS)
    def _(n):
        end_waits(n)

    sends = [
        (TO_SIB, True), (TO_OPP, True), (FWD, True),
        (UP, v <= 1), (DOWN, (v == 1) | (v == 3)), (DOWN_OPP, v == 1),
        (UP_OPP, lift), (UP_DIA, lift),
        (HOP_OWN, hop0 | hop1), (HOP_SIB, hop0 | hop1), (HOP_OPP, hop1), (HOP_DIA, hop1),
        (PASS, (v == 1) | (v == 2)), (CROSS, v <= 2),
    ]

    @pl.loop(0, CHUNKS)
    def _(c):
        for kind, cond in sends:
            when(cond, lambda: copy(at(x, 0, c), at(xz, 0, c), send.at[kind, c], rz.at[0, c], to_sib).wait_send())


def gather(pair_block, weights):
    rows, cols = pair_block.shape
    width = cols // UNITS
    bf16 = jnp.bfloat16
    full = jax.ShapeDtypeStruct((4 * rows, cols), bf16)
    return pl.pallas_call(
        gather_kernel,
        out_shape=(
            full,
            full,
            jax.ShapeDtypeStruct((rows, cols), bf16),
            pltpu.VMEM((cols, 4 * rows), bf16),
            pltpu.VMEM((cols, EARLY * width), bf16),
        ),
        in_specs=[pl.BlockSpec(memory_space=pl.ANY), pl.BlockSpec(memory_space=pltpu.VMEM)],
        out_specs=[pl.BlockSpec(memory_space=m) for m in (pltpu.HBM,) * 3 + (pltpu.VMEM,) * 2],
        scratch_shapes=[
            pltpu.VMEM((rows, cols), bf16),
            pltpu.VMEM((2, 4 * rows, width), bf16),
            pltpu.SemaphoreType.DMA((14, CHUNKS)),
            pltpu.SemaphoreType.DMA((4, CHUNKS)),
            pltpu.SemaphoreType.DMA((4, CHUNKS)),
            pltpu.SemaphoreType.DMA((1, CHUNKS)),
            pltpu.SemaphoreType.DMA((1,)),
            pltpu.SemaphoreType.DMA((2, 4)),
        ],
        compiler_params=pltpu.CompilerParams(collective_id=0, has_side_effects=True, vmem_limit_bytes=13 * MIB),
    )(pair_block, weights[None, :])


def finish_kernel(x, xz, xb, lhs, kept, out, rhs, acc, hold, rhs_sem, acc_sem, out_sem):
    rows, cols = x.shape
    width, tile = cols // UNITS, cols // TILES
    strip = tile // STRIPS
    done = EARLY * width
    b, z, y, k, u, v = place()

    def span(i, size):
        return pl.ds(pl.multiple_of(i * size, size), size)

    def put(i):
        s = lax.rem(i, SLOTS)
        return pltpu.make_async_copy(hold.at[s], out.at[span(i, strip), pl.ds(0, done)], out_sem.at[s])

    def store(p):
        s = lax.rem(p, 2)
        return pltpu.make_async_copy(acc.at[s], out.at[span(p, tile), pl.ds(done, width)], acc_sem.at[s])

    load_columns(x, xz, xb, rhs, rhs_sem, u == v, b, EARLY, width)

    @pl.loop(0, TILES)
    def _(p):
        for j in range(STRIPS):
            i = p * STRIPS + j
            pl.when(i >= SLOTS)(lambda: put(i - SLOTS).wait())
            hold[lax.rem(i, SLOTS)] = kept[span(i, strip), :].astype(jnp.float32)
            put(i).start()
        pl.when(p == 0)(lambda: await_columns(xb, rhs, rhs_sem, rows, width))
        pl.when(p >= 2)(lambda: store(p - 2).wait())
        acc[lax.rem(p, 2)] = jnp.dot(lhs[span(p, tile), :], rhs[...], preferred_element_type=jnp.float32)
        store(p).start()

    for p in range(TILES - 2, TILES):
        store(p).wait()
    for i in range(TILES * STRIPS - SLOTS, TILES * STRIPS):
        put(i).wait()


def finish(pair_block, xz, xb, lhs, kept):
    rows, cols = pair_block.shape
    width, tile = cols // UNITS, cols // TILES
    bf16, f32 = jnp.bfloat16, jnp.float32
    lhs = pltpu.with_memory_space_constraint(lhs, pltpu.VMEM)
    kept = pltpu.with_memory_space_constraint(kept, pltpu.VMEM)
    return pl.pallas_call(
        finish_kernel,
        out_shape=jax.ShapeDtypeStruct((cols, cols), f32),
        in_specs=[pl.BlockSpec(memory_space=m) for m in (pl.ANY,) * 3 + (pltpu.VMEM,) * 2],
        out_specs=pl.BlockSpec(memory_space=pl.ANY),
        scratch_shapes=[
            pltpu.VMEM((4 * rows, width), bf16),
            pltpu.VMEM((2, tile, width), f32),
            pltpu.VMEM((SLOTS, tile // STRIPS, EARLY * width), f32),
            pltpu.SemaphoreType.DMA((4,)),
            pltpu.SemaphoreType.DMA((2,)),
            pltpu.SemaphoreType.DMA((SLOTS,)),
        ],
        compiler_params=pltpu.CompilerParams(vmem_limit_bytes=17 * MIB),
    )(pair_block, xz, xb, lhs, kept)


def shards(square, pair_block, occ_energy, virt_energy, frequency):
    weights = pair_weights(occ_energy, virt_energy, frequency)
    if square:
        xz, xb, _, lhs, kept = gather(pair_block, weights)
        return finish(pair_block, xz, xb, lhs, kept)
    row_full = lax.all_gather(pair_block, "col", axis=1, tiled=True)
    column_slab = lax.all_to_all(row_full, "blk", split_axis=1, concat_axis=0, tiled=True)
    own_columns = lax.all_gather(pair_block, "blk", axis=0, tiled=True)
    scaled = (own_columns.astype(jnp.float32) * weights[:, None]).astype(jnp.bfloat16)
    return lax.dot_general(
        scaled, column_slab, (((0,), (0,)), ((), ())), preferred_element_type=jnp.float32
    )


def solution(mesh):
    square = mesh.shape["blk"] == 4 and mesh.shape["col"] == 4
    return jax.shard_map(
        functools.partial(shards, square),
        mesh=mesh,
        in_specs=(P(("groups", "blk"), "col"), P("groups"), P("groups"), P("groups")),
        out_specs=P(("groups", "col"), "blk"),
        check_vma=False,
    )
```

```python
import functools

import jax
import jax.numpy as jnp
from jax import lax
from jax.experimental import pallas as pl
from jax.experimental.pallas import tpu as pltpu
from jax.sharding import PartitionSpec as P

MESH = pl.DeviceIdType.MESH
CHUNKS = 32
UNITS = 16
TILES = 8
EARLY = 13
FIRST = CHUNKS + 11
HELD = 3 * CHUNKS // 4
TICKS = 3 * CHUNKS + 4
PER_TICK = 64 // CHUNKS
SPAN = TILES // PER_TICK
MIB = 1 << 20
TAIL = CHUNKS // 16
CUT = CHUNKS - TAIL
TO_SIB, TO_OPP, UP, DOWN, FWD, DOWN_OPP, UP_OPP, UP_DIA, HOP_OWN, HOP_SIB, HOP_OPP, HOP_DIA, PASS, CROSS, SIDE, SIDE_CROSS = range(16)
SLOTS = 6
STRIPS = 4


def aside(c):
    return (c >= CUT - 7) & (c < CUT - 1)


def pair_weights(occ_energy, virt_energy, frequency):
    gap = (virt_energy[None, :] - occ_energy[:, None]).reshape(-1)
    return 2.0 * gap / (gap * gap + frequency[0] * frequency[0])


def place():
    b, z = lax.axis_index("blk"), lax.axis_index("col")
    last = lax.axis_size("col") - 1
    y, k = b // 2, b % 2
    u, v = k + y - 2 * y * k, z + y * (last - 2 * z)
    return b, z, y, k, u, v


def load_columns(x, xz, xb, dst, sem, at_home, own, n, width, count=1):
    rows = x.shape[0]
    cols = pl.ds(pl.multiple_of(n * width, width), count * width)

    def piece(src, r):
        return pltpu.make_async_copy(src, dst.at[pl.ds(pl.multiple_of(r * rows, rows), rows)], sem.at[r])

    for r in range(4):
        band = pl.ds(r * rows, rows)

        @pl.when(jnp.logical_not(at_home))
        def _():
            piece(xb.at[band, cols], r).start()

        @pl.when(at_home & (own != r))
        def _():
            piece(xz.at[band, cols], r).start()

        @pl.when(at_home & (own == r))
        def _():
            piece(x.at[:, cols], r).start()


def await_columns(xb, dst, sem, rows, width):
    for r in range(4):
        band = pl.ds(r * rows, rows)
        pltpu.make_async_copy(xb.at[band, pl.ds(0, width)], dst.at[band], sem.at[r]).wait()


def gather_kernel(
    x, occ, virt, freq, xz, xb, tr, ts, tail_h, tail_o, lhs_out, lhs, kept,
    stage, rhs, wt, send, rz, rb, rt, rs, stage_sem, rhs_sem, tail_sem, lhs_sem,
):
    rows, cols = x.shape
    step = cols // CHUNKS
    width = cols // UNITS
    tile = cols // TILES
    g = lax.axis_index("groups")
    b, z, y, k, u, v = place()
    dz = 1 - 2 * y
    own, sib, opp, dia = b, 2 * y + 1 - k, 2 * (1 - y) + k, 2 * (1 - y) + 1 - k
    lead0, lead1 = 3 * y, y + 1
    at_home = u == v

    def at(ref, r, c):
        return ref.at[
            pl.ds(pl.multiple_of(r * rows, rows), rows), pl.ds(pl.multiple_of(c * step, step), step)
        ]

    def copy(src, dst, ssem, rsem, dev):
        return pltpu.make_async_remote_copy(
            src_ref=src, dst_ref=dst, send_sem=ssem, recv_sem=rsem, device_id=(g, dev[0], dev[1]), device_id_type=MESH
        )

    to_sib, to_opp = (sib, z), (opp, z)
    up0, up1 = (lead0, z + dz), (lead1, z + dz)
    down1, down_same = (lead1, z - dz), (b, z - dz)
    across = (3 * (1 - y), z)

    def go(kind, c, src, ref, rsem, r, dev):
        copy(src, at(ref, r, c), send.at[kind], rsem.at[r, c], dev).start()

    def arrived(ref, rsem, r, c):
        copy(at(ref, r, c), at(ref, r, c), send.at[0], rsem.at[r, c], to_sib).wait_recv()

    hop0 = (u == 0) & ((v == 1) | (v == 2))
    hop1 = (u == 1) & (v == 2)
    lift = (v == 1) & (u == 1)

    barrier = pltpu.get_barrier_semaphore()
    last = lax.axis_size("col") - 1

    def greet(dev):
        pl.semaphore_signal(barrier, inc=1, device_id=(g,) + dev, device_id_type=MESH)

    for dev in ((sib, z), (opp, z), (dia, z)):
        greet(dev)
    for core in (own, sib):
        pl.when(z > 0)(lambda: greet((core, z - 1)))
        pl.when(z < last)(lambda: greet((core, z + 1)))
    pl.semaphore_wait(barrier, 3 + 2 * (z > 0).astype(jnp.int32) + 2 * (z < last).astype(jnp.int32))

    homes = [(own, tail_h, k), (sib, tail_h, 1 - k), (opp, tail_o, k), (dia, tail_o, 1 - k)]

    def tail_at(r, c):
        ref, i = next((ref, i) for key, ref, i in homes if key is r)
        return ref.at[
            pl.ds(pl.multiple_of(i * rows, rows), rows), pl.ds(pl.multiple_of((c - CUT) * step, step), step)
        ]

    def go_xb(kind, c, src, r, dev):
        def main():
            copy(src, at(xb, r, c), send.at[kind], rb.at[r, c], dev).start()

        def tail():
            copy(src, tail_at(r, c), send.at[kind], rb.at[r, c], dev).start()

        if isinstance(c, int):
            main()
        else:
            pl.when(c < CUT)(main)
            pl.when(c >= CUT)(tail)

    def line_own(c):
        src = at(x, 0, c)
        pl.when(v == 1)(lambda: go_xb(UP, c, src, own, up1))
        pl.when((v == 1) & (c < HELD))(lambda: go(DOWN, c, src, xb, rb, own, down1))

    line_own(0)
    line_own(1)

    @pl.loop(0, CHUNKS)
    def _(c):
        src = at(x, 0, c)
        go(TO_OPP, c, src, xz, rz, own, to_opp)
        pl.when(v == 0)(lambda: go_xb(UP, c, src, own, up0))
        pl.when(v == 3)(lambda: go(DOWN, c, src, tr, rt, 0, down_same))
        go(TO_SIB, c, src, xz, rz, own, to_sib)

    def hop(kind, r, c, dev):
        arrived(xb, rb, r, c)

        @pl.when(c < CUT)
        def _():
            go(kind, c, at(xb, r, c), xb, rb, r, dev)

        @pl.when((c >= CUT) & (v == 1))
        def _():
            go_tail = copy(tail_at(r, c), tail_at(r, c), send.at[kind], rb.at[r, c], dev)
            go_tail.start()

    def end_waits(n):
        for i in range(CHUNKS // UNITS):
            c = n * (CHUNKS // UNITS) + i
            for r in (own, sib):
                pl.when(jnp.logical_not(at_home | hop0 | hop1) & (c < CUT))(lambda: arrived(xb, rb, r, c))
            for r in (opp, dia):
                pl.when(jnp.logical_not(at_home | hop1) & ((c < CUT) | (u == 0)))(lambda: arrived(xb, rb, r, c))

    def stage_load(src):
        return pltpu.make_async_copy(src, stage, stage_sem.at[0])

    def band(ref, r):
        return ref.at[pl.ds(pl.multiple_of(r * rows, rows), rows)]

    def go_across(kind, c, src, dev):
        @pl.when(c < CUT)
        def _():
            go(kind, c, src, xb, rb, own, dev)

        @pl.when(c >= CUT)
        def _():
            copy(src, tail_at(opp, c), send.at[kind], rb.at[own, c], dev).start()

    def rest(ref, half):
        r = pl.ds(pl.multiple_of(half * 2 * rows, 2 * rows), 2 * rows)
        return rhs.at[0, r, pl.ds(0, TAIL * step)]

    lhs_save = pltpu.make_async_copy(lhs, lhs_out, lhs_sem.at[0])

    for i in range(occ.shape[0]):
        gap = virt[...] - occ[i]
        wt[:, pl.ds(i * virt.shape[1], virt.shape[1])] = 2.0 * gap / (gap * gap + freq[0] * freq[0])

    @pl.loop(0, TICKS)
    def _(t):
        m, phase = t // 3, lax.rem(t, 3)

        @pl.when((t + 2 < CHUNKS) & (t >= 0))
        def _():
            line_own(t + 2)

        @pl.when(t < CHUNKS)
        def _():
            arrived(xz, rz, opp, t)
            src = at(xz, opp, t)
            pl.when(lift & jnp.logical_not(aside(t)))(lambda: go_xb(UP_OPP, t, src, opp, up1))
            pl.when((v == 1) & (t < HELD))(lambda: go(DOWN_OPP, t, src, xb, rb, opp, down1))
            go(FWD, t, src, xz, rz, opp, to_sib)

            @pl.when((u == 0) & (v == 1))
            def _():
                hop(HOP_OWN, own, t, up0)
                hop(HOP_SIB, sib, t, up0)

        @pl.when((t >= 1) & (t < CHUNKS + 1))
        def _():
            arrived(xz, rz, dia, t - 1)

            @pl.when(lift & jnp.logical_not(aside(t - 1)))
            def _():
                go_xb(UP_DIA, t - 1, at(xz, dia, t - 1), dia, up1)

        held = HELD + t - (CHUNKS + 2)

        @pl.when((v == 1) & (held >= HELD) & (held < CUT))
        def _():
            go(DOWN, held, at(x, 0, held), xb, rb, own, down1)
            go(DOWN_OPP, held, at(xz, opp, held), xb, rb, opp, down1)

        slow, burst = m - 2, t - 2 * HELD
        late = jnp.where(v == 0, jnp.where(burst >= HELD - 3, burst, slow), t - 2 + v)
        paced = (v > 0) | ((phase == 1) & (slow < HELD - 3)) | (burst >= HELD - 3)

        @pl.when((v <= 2) & paced & (late >= 0) & (late < CHUNKS))
        def _():
            arrived(tr, rt, 0, late)
            src = at(tr, 0, late)
            pl.when(v >= 1)(lambda: go(PASS, late, src, tr, rt, 0, down_same))
            go_across(CROSS, late, src, across)

        @pl.when((v == 2) & (t == CHUNKS // 2))
        def _():
            @pl.loop(0, CHUNKS)
            def _(c):
                pl.when(aside(c))(lambda: go(SIDE, c, at(x, 0, c), ts, rs, 0, down_same))

        side = t - (CHUNKS + 2) + CUT - 7

        @pl.when((v == 1) & (t >= CHUNKS + 2) & aside(side))
        def _():
            arrived(ts, rs, 0, side)
            go(SIDE_CROSS, side, at(ts, 0, side), xb, rb, own, (2 - y, z))

        @pl.when(hop1)
        def _():
            @pl.when((phase == 0) & (m >= 2) & (m < CHUNKS + 2))
            def _():
                hop(HOP_DIA, dia, m - 2, up1)

            @pl.when(t < 2)
            def _():
                hop(HOP_OWN, own, t, up1)
                hop(HOP_SIB, sib, t, up1)

            @pl.when((phase == 1) & (m < CHUNKS - 2))
            def _():
                hop(HOP_OWN, own, m + 2, up1)

            @pl.when((phase == 2) & (m < CHUNKS - 2))
            def _():
                hop(HOP_SIB, sib, m + 2, up1)

            @pl.when((phase == 2) & (m < CHUNKS))
            def _():
                hop(HOP_OPP, opp, m, up1)

        @pl.when((u == 0) & (v == 2) & (m >= 1) & (m <= CHUNKS))
        def _():
            pl.when(phase == 0)(lambda: hop(HOP_OWN, own, m - 1, up0))
            pl.when(phase == 1)(lambda: hop(HOP_SIB, sib, m - 1, up0))

        @pl.when(t == 9)
        def _():
            @pl.loop(0, CHUNKS)
            def _(c):
                arrived(xz, rz, sib, c)

        @pl.when(at_home & (t == CHUNKS + 5))
        def _():
            near = rhs.at[0, :, pl.ds(0, TAIL * step)]
            load_columns(x, xz, xb, near, rhs_sem.at[0], at_home, own, CUT // TAIL, TAIL * step)
            await_columns(xb, near, rhs_sem.at[0], rows, TAIL * step)
            saves = [
                pltpu.make_async_copy(rest(tail_h, y), tail_h, tail_sem.at[0]),
                pltpu.make_async_copy(rest(tail_o, 1 - y), tail_o, tail_sem.at[1]),
            ]
            for save in saves:
                save.start()
            for save in saves:
                save.wait()

        fill = (t == 3) | (t == 10) | (t == CHUNKS + 1) | (t == CHUNKS + 2)

        @pl.when(fill)
        def _():
            r = jnp.where(t == 3, own, jnp.where(t == 10, sib, jnp.where(t == CHUNKS + 1, opp, dia)))
            stage_load(x).wait()
            scale = wt[:, pl.ds(pl.multiple_of(r * rows, rows), rows)]

            @pl.loop(0, TILES)
            def _(i):
                p = pl.ds(pl.multiple_of(i * tile, tile), tile)
                turned = stage[:, p].T.astype(jnp.float32) * scale
                lhs[p, pl.ds(pl.multiple_of(r * rows, rows), rows)] = turned.astype(jnp.bfloat16)

        pl.when(t == CHUNKS + 3)(lambda: lhs_save.start())
        pl.when(t == 1)(lambda: stage_load(x).start())
        pl.when(t == 9)(lambda: stage_load(band(xz, sib)).start())
        pl.when(t == CHUNKS)(lambda: stage_load(band(xz, opp)).start())
        pl.when(t == CHUNKS + 1)(lambda: stage_load(band(xz, dia)).start())

        work = t - FIRST
        n, q = work // SPAN, lax.rem(work, SPAN)

        @pl.when((work >= 0) & (work < SPAN * EARLY))
        def _():
            s = lax.rem(n, 2)

            @pl.when(q == 0)
            def _():
                await_columns(xb, rhs.at[s], rhs_sem.at[s], rows, width)

            for j in range(PER_TICK):
                p = PER_TICK * q + j
                got = jnp.dot(
                    lhs[pl.ds(pl.multiple_of(p * tile, tile), tile), :], rhs[s], preferred_element_type=jnp.float32
                )
                kept[
                    pl.ds(pl.multiple_of(p * tile, tile), tile), pl.ds(pl.multiple_of(n * width, width), width)
                ] = got.astype(jnp.bfloat16)

        ahead = work + 1
        n_ahead = ahead // SPAN

        @pl.when((ahead >= 0) & (ahead < SPAN * EARLY) & (lax.rem(ahead, SPAN) == 0))
        def _():
            end_waits(n_ahead)
            s = lax.rem(n_ahead, 2)
            load_columns(x, xz, xb, rhs.at[s], rhs_sem.at[s], at_home, own, n_ahead, width)

    def drain(kind, count):
        sent = x.at[:, pl.ds(0, count * step)]
        copy(sent, sent, send.at[kind], rz.at[0, 0], to_sib).wait_send()

    def drain_if(cond, kind, count):
        pl.when(cond)(lambda: drain(kind, count))

    def finals():
        @pl.loop(EARLY, UNITS)
        def _(n):
            end_waits(n)

    few = CUT - 1 - (CUT - 7)
    lhs_save.wait()
    for kind in (TO_SIB, TO_OPP, FWD):
        drain(kind, CHUNKS)
    drain_if(v == 2, SIDE, few)
    drain_if(v == 1, SIDE_CROSS, few)
    drain_if(v <= 2, CROSS, CHUNKS)
    drain_if((v == 1) | (v == 2), PASS, CHUNKS)
    drain_if(v == 0, UP, CHUNKS)
    drain_if(v == 3, DOWN, CHUNKS)
    finals()
    drain_if(v == 1, UP, CHUNKS)
    for kind in (UP_OPP, UP_DIA):
        drain_if(lift, kind, CHUNKS - few)
    for kind in (DOWN, DOWN_OPP):
        drain_if(v == 1, kind, CUT)
    for kind in (HOP_OWN, HOP_SIB):
        drain_if((u == 0) & (v == 1), kind, CHUNKS)
        drain_if(v == 2, kind, CUT)
    for kind in (HOP_OPP, HOP_DIA):
        drain_if(hop1, kind, CUT)


def gather(pair_block, occ_energy, virt_energy, frequency):
    rows, cols = pair_block.shape
    width, narrow = cols // UNITS, cols * TAIL // CHUNKS
    bf16 = jnp.bfloat16
    full = jax.ShapeDtypeStruct((4 * rows, cols), bf16)
    block = jax.ShapeDtypeStruct((rows, cols), bf16)
    half = jax.ShapeDtypeStruct((2 * rows, narrow), bf16)
    return pl.pallas_call(
        gather_kernel,
        out_shape=(
            full, full, block, block, half, half,
            jax.ShapeDtypeStruct((cols, 4 * rows), bf16),
            pltpu.VMEM((cols, 4 * rows), bf16),
            pltpu.VMEM((cols, EARLY * width), bf16),
        ),
        in_specs=[pl.BlockSpec(memory_space=m) for m in (pl.ANY, pltpu.SMEM, pltpu.VMEM, pltpu.SMEM)],
        out_specs=[pl.BlockSpec(memory_space=m) for m in (pltpu.HBM,) * 7 + (pltpu.VMEM,) * 2],
        scratch_shapes=[
            pltpu.VMEM((rows, cols), bf16),
            pltpu.VMEM((2, 4 * rows, width), bf16),
            pltpu.VMEM((1, 4 * rows), jnp.float32),
            pltpu.SemaphoreType.DMA((16,)),
            pltpu.SemaphoreType.DMA((4, CHUNKS)),
            pltpu.SemaphoreType.DMA((4, CHUNKS)),
            pltpu.SemaphoreType.DMA((1, CHUNKS)),
            pltpu.SemaphoreType.DMA((1, CHUNKS)),
            pltpu.SemaphoreType.DMA((1,)),
            pltpu.SemaphoreType.DMA((2, 4)),
            pltpu.SemaphoreType.DMA((2,)),
            pltpu.SemaphoreType.DMA((1,)),
        ],
        compiler_params=pltpu.CompilerParams(collective_id=0, has_side_effects=True, vmem_limit_bytes=13 * MIB),
    )(pair_block, occ_energy, virt_energy[None, :], frequency)


def span(i, size):
    return pl.ds(pl.multiple_of(i * size, size), size)


def finish_kernel(x, xz, xb, lhs, kept, out, rhs, acc, hold, rhs_sem, acc_sem, out_sem):
    rows, cols = x.shape
    width, tile, narrow = cols // UNITS, cols // TILES, cols * TAIL // CHUNKS
    strip = tile // STRIPS
    done = EARLY * width
    mid = cols - narrow - done
    b, z, y, k, u, v = place()

    def put(i):
        s = lax.rem(i, SLOTS)
        return pltpu.make_async_copy(hold.at[s], out.at[span(i, strip), pl.ds(0, done)], out_sem.at[s])

    def store(p):
        s = lax.rem(p, 2)
        cut = pl.ds(done, mid)
        return pltpu.make_async_copy(acc.at[s], out.at[span(p, tile), cut], acc_sem.at[s])

    load_columns(x, xz, xb, rhs, rhs_sem, u == v, b, EARLY, width, mid // width)

    @pl.loop(0, TILES)
    def _(p):
        for j in range(STRIPS):
            i = p * STRIPS + j
            pl.when(i >= SLOTS)(lambda: put(i - SLOTS).wait())
            hold[lax.rem(i, SLOTS)] = kept[span(i, strip), :].astype(jnp.float32)
            put(i).start()
        pl.when(p == 0)(lambda: await_columns(xb, rhs, rhs_sem, rows, mid))
        pl.when(p >= 2)(lambda: store(p - 2).wait())
        acc[lax.rem(p, 2)] = jnp.dot(lhs[span(p, tile), :], rhs[...], preferred_element_type=jnp.float32)
        store(p).start()

    for p in range(TILES - 2, TILES):
        store(p).wait()
    for i in range(TILES * STRIPS - SLOTS, TILES * STRIPS):
        put(i).wait()


def finish(pair_block, xz, xb, lhs, kept):
    rows, cols = pair_block.shape
    width, tile, narrow = cols // UNITS, cols // TILES, cols * TAIL // CHUNKS
    mid = cols - narrow - EARLY * width
    bf16, f32 = jnp.bfloat16, jnp.float32
    return pl.pallas_call(
        finish_kernel,
        out_shape=jax.ShapeDtypeStruct((cols, cols), f32),
        in_specs=[pl.BlockSpec(memory_space=m) for m in (pl.ANY,) * 3 + (pltpu.VMEM,) * 2],
        out_specs=pl.BlockSpec(memory_space=pl.ANY),
        scratch_shapes=[
            pltpu.VMEM((4 * rows, mid), bf16),
            pltpu.VMEM((2, tile, mid), f32),
            pltpu.VMEM((SLOTS, tile // STRIPS, EARLY * width), f32),
            pltpu.SemaphoreType.DMA((4,)),
            pltpu.SemaphoreType.DMA((2,)),
            pltpu.SemaphoreType.DMA((SLOTS,)),
        ],
        cost_estimate=pl.CostEstimate(flops=10**10, bytes_accessed=cols * cols * 4, transcendentals=0),
        compiler_params=pltpu.CompilerParams(vmem_limit_bytes=16 * MIB),
    )(pair_block, xz, xb, lhs, kept)


def tail_kernel(lhs_in, tail_h, tail_o, got_h, got_o, _, out, lhs, rhs, acc, lhs_sem, rhs_sem, acc_sem):
    cols = out.shape[0]
    tile, narrow = cols // TILES, rhs.shape[1]
    half = tail_h.shape[0]
    b, z, y, k, u, v = place()
    parts = [(tail_h, got_h, y, (v == 3) | ((v == 0) & (u == 1))), (tail_o, got_o, 1 - y, (u == 1) & ((v == 3) | (v == 0)))]

    def fetch(src, at, i):
        return pltpu.make_async_copy(src, rhs.at[pl.ds(pl.multiple_of(at * half, half), half)], rhs_sem.at[i])

    def store(p):
        s = lax.rem(p, 2)
        return pltpu.make_async_copy(acc.at[s], out.at[span(p, tile), pl.ds(cols - narrow, narrow)], acc_sem.at[s])

    def turn(p):
        return pltpu.make_async_copy(lhs_in.at[span(p, tile)], lhs.at[lax.rem(p, 3)], lhs_sem.at[lax.rem(p, 3)])

    turn(0).start()
    for i, (near, far, at, remote) in enumerate(parts):
        pl.when(remote)(lambda: fetch(far, at, i).start())
        pl.when(jnp.logical_not(remote))(lambda: fetch(near, at, i).start())
    turn(1).start()
    for i, (near, far, at, remote) in enumerate(parts):
        fetch(near, at, i).wait()

    @pl.loop(0, TILES)
    def _(p):
        turn(p).wait()
        pl.when(p + 2 < TILES)(lambda: turn(p + 2).start())
        pl.when(p >= 2)(lambda: store(p - 2).wait())
        acc[lax.rem(p, 2)] = jnp.dot(lhs[lax.rem(p, 3)], rhs[...], preferred_element_type=jnp.float32)
        store(p).start()

    for p in range(TILES - 2, TILES):
        store(p).wait()


def close(lhs, tail_h, tail_o, got_h, got_o, out):
    cols, depth = lhs.shape
    tile, narrow = cols // TILES, tail_h.shape[1]
    return pl.pallas_call(
        tail_kernel,
        out_shape=jax.ShapeDtypeStruct(out.shape, out.dtype),
        in_specs=[pl.BlockSpec(memory_space=m) for m in (pl.ANY,) * 6],
        out_specs=pl.BlockSpec(memory_space=pl.ANY),
        scratch_shapes=[
            pltpu.VMEM((3, tile, depth), jnp.bfloat16),
            pltpu.VMEM((depth, narrow), jnp.bfloat16),
            pltpu.VMEM((2, tile, narrow), jnp.float32),
            pltpu.SemaphoreType.DMA((3,)),
            pltpu.SemaphoreType.DMA((2,)),
            pltpu.SemaphoreType.DMA((2,)),
        ],
        input_output_aliases={5: 0},
        compiler_params=pltpu.CompilerParams(vmem_limit_bytes=52 * MIB),
    )(lhs, tail_h, tail_o, got_h, got_o, out)


def last_hops(groups):
    def index(g, b, z):
        return (g * 4 + b) * 4 + z

    both, lone = [], []
    for i in range(groups * 16):
        g, b, z = i // 16, i // 4 % 4, i % 4
        y, k = b // 2, b % 2
        u, v = k + y - 2 * y * k, z + y * (3 - 2 * z)
        d = 1 - 2 * y
        if v == 2:
            both.append((i, index(g, b, z + d)))
            if u == 1:
                lone.append((i, index(g, b, z + d)))
        if v == 1 and u == 1:
            both.append((i, index(g, b, z - d)))
            lone.append((i, index(g, b, z - d)))
    return both, lone


def shards(square, groups, pair_block, occ_energy, virt_energy, frequency):
    if square:
        xz, xb, _, _, tail_h, tail_o, lhs_back, lhs, kept = gather(pair_block, occ_energy, virt_energy, frequency)
        both, lone = last_hops(groups)
        axes = ("groups", "blk", "col")
        got_h = lax.ppermute(tail_h, axes, both)
        got_o = lax.ppermute(tail_o, axes, lone)
        lhs = pltpu.with_memory_space_constraint(lhs, pltpu.VMEM)
        kept = pltpu.with_memory_space_constraint(kept, pltpu.VMEM)
        out = finish(pair_block, xz, xb, lhs, kept)
        return close(lhs_back, tail_h, tail_o, got_h, got_o, out)
    weights = pair_weights(occ_energy, virt_energy, frequency)
    row_full = lax.all_gather(pair_block, "col", axis=1, tiled=True)
    column_slab = lax.all_to_all(row_full, "blk", split_axis=1, concat_axis=0, tiled=True)
    own_columns = lax.all_gather(pair_block, "blk", axis=0, tiled=True)
    scaled = (own_columns.astype(jnp.float32) * weights[:, None]).astype(jnp.bfloat16)
    return lax.dot_general(
        scaled, column_slab, (((0,), (0,)), ((), ())), preferred_element_type=jnp.float32
    )


def solution(mesh):
    square = mesh.shape["blk"] == 4 and mesh.shape["col"] == 4
    return jax.shard_map(
        functools.partial(shards, square, mesh.shape["groups"]),
        mesh=mesh,
        in_specs=(P(("groups", "blk"), "col"), P("groups"), P("groups"), P("groups")),
        out_specs=P(("groups", "col"), "blk"),
        check_vma=False,
    )
```

```python
import functools

import jax
import jax.numpy as jnp
from jax import lax
from jax.experimental import pallas as pl
from jax.experimental.pallas import tpu as pltpu
from jax.sharding import PartitionSpec as P

MESH = pl.DeviceIdType.MESH
CHUNKS = 32
UNITS = 16
TILES = 8
EARLY = 13
FIRST = CHUNKS + 7
HELD = 3 * CHUNKS // 4
TICKS = 3 * CHUNKS + 4
PER_TICK = 64 // CHUNKS
SPAN = TILES // PER_TICK
MIB = 1 << 20
TAIL = CHUNKS // 16
CUT = CHUNKS - TAIL
TO_SIB, TO_OPP, UP, DOWN, FWD, DOWN_OPP, UP_OPP, UP_DIA, HOP_OWN, HOP_SIB, HOP_OPP, HOP_DIA, PASS, CROSS, SIDE, SIDE_CROSS = range(16)
SLOTS = 7
STRIPS = 4


def aside(c):
    return (c >= CUT - 7) & (c < CUT - 1)


def pair_weights(occ_energy, virt_energy, frequency):
    gap = (virt_energy[None, :] - occ_energy[:, None]).reshape(-1)
    return 2.0 * gap / (gap * gap + frequency[0] * frequency[0])


def place():
    b, z = lax.axis_index("blk"), lax.axis_index("col")
    last = lax.axis_size("col") - 1
    y, k = b // 2, b % 2
    u, v = k + y - 2 * y * k, z + y * (last - 2 * z)
    return b, z, y, k, u, v


def load_columns(x, xz, xb, dst, sem, at_home, own, n, width, count=1):
    rows = x.shape[0]
    cols = pl.ds(pl.multiple_of(n * width, width), count * width)

    def piece(src, r):
        return pltpu.make_async_copy(src, dst.at[pl.ds(pl.multiple_of(r * rows, rows), rows)], sem.at[r])

    for r in range(4):
        band = pl.ds(r * rows, rows)

        @pl.when(jnp.logical_not(at_home))
        def _():
            piece(xb.at[band, cols], r).start()

        @pl.when(at_home & (own != r))
        def _():
            piece(xz.at[band, cols], r).start()

        @pl.when(at_home & (own == r))
        def _():
            piece(x.at[:, cols], r).start()


def await_columns(xb, dst, sem, rows, width):
    for r in range(4):
        band = pl.ds(r * rows, rows)
        pltpu.make_async_copy(xb.at[band, pl.ds(0, width)], dst.at[band], sem.at[r]).wait()


def gather_kernel(
    x, occ, virt, freq, xz, xb, tr, ts, tail_h, tail_o, lhs_out, lhs, kept,
    stage, rhs, wt, send, rz, rb, rt, rs, stage_sem, rhs_sem, tail_sem, lhs_sem,
):
    rows, cols = x.shape
    step = cols // CHUNKS
    width = cols // UNITS
    tile = cols // TILES
    g = lax.axis_index("groups")
    b, z, y, k, u, v = place()
    dz = 1 - 2 * y
    own, sib, opp, dia = b, 2 * y + 1 - k, 2 * (1 - y) + k, 2 * (1 - y) + 1 - k
    lead0, lead1 = 3 * y, y + 1
    at_home = u == v

    def at(ref, r, c):
        return ref.at[
            pl.ds(pl.multiple_of(r * rows, rows), rows), pl.ds(pl.multiple_of(c * step, step), step)
        ]

    def copy(src, dst, ssem, rsem, dev):
        return pltpu.make_async_remote_copy(
            src_ref=src, dst_ref=dst, send_sem=ssem, recv_sem=rsem, device_id=(g, dev[0], dev[1]), device_id_type=MESH
        )

    to_sib, to_opp = (sib, z), (opp, z)
    up0, up1 = (lead0, z + dz), (lead1, z + dz)
    down1, down_same = (lead1, z - dz), (b, z - dz)
    across = (3 * (1 - y), z)

    def go(kind, c, src, ref, rsem, r, dev):
        copy(src, at(ref, r, c), send.at[kind], rsem.at[r, c], dev).start()

    def arrived(ref, rsem, r, c):
        copy(at(ref, r, c), at(ref, r, c), send.at[0], rsem.at[r, c], to_sib).wait_recv()

    hop0 = (u == 0) & ((v == 1) | (v == 2))
    hop1 = (u == 1) & (v == 2)
    lift = (v == 1) & (u == 1)

    barrier = pltpu.get_barrier_semaphore()
    last = lax.axis_size("col") - 1

    def greet(dev):
        pl.semaphore_signal(barrier, inc=1, device_id=(g,) + dev, device_id_type=MESH)

    for dev in ((sib, z), (opp, z), (dia, z)):
        greet(dev)
    for core in (own, sib):
        pl.when(z > 0)(lambda: greet((core, z - 1)))
        pl.when(z < last)(lambda: greet((core, z + 1)))
    pl.semaphore_wait(barrier, 3 + 2 * (z > 0).astype(jnp.int32) + 2 * (z < last).astype(jnp.int32))

    homes = [(own, tail_h, k), (sib, tail_h, 1 - k), (opp, tail_o, k), (dia, tail_o, 1 - k)]

    def tail_at(r, c):
        ref, i = next((ref, i) for key, ref, i in homes if key is r)
        return ref.at[
            pl.ds(pl.multiple_of(i * rows, rows), rows), pl.ds(pl.multiple_of((c - CUT) * step, step), step)
        ]

    def go_xb(kind, c, src, r, dev):
        def main():
            copy(src, at(xb, r, c), send.at[kind], rb.at[r, c], dev).start()

        def tail():
            copy(src, tail_at(r, c), send.at[kind], rb.at[r, c], dev).start()

        if isinstance(c, int):
            main()
        else:
            pl.when(c < CUT)(main)
            pl.when(c >= CUT)(tail)

    def line_own(c):
        src = at(x, 0, c)
        pl.when(v == 1)(lambda: go_xb(UP, c, src, own, up1))
        pl.when((v == 1) & (c < HELD))(lambda: go(DOWN, c, src, xb, rb, own, down1))

    line_own(0)
    line_own(1)

    @pl.loop(0, CHUNKS)
    def _(c):
        src = at(x, 0, c)
        go(TO_OPP, c, src, xz, rz, own, to_opp)
        pl.when(v == 0)(lambda: go_xb(UP, c, src, own, up0))
        pl.when(v == 3)(lambda: go(DOWN, c, src, tr, rt, 0, down_same))
        go(TO_SIB, c, src, xz, rz, own, to_sib)

    def hop(kind, r, c, dev):
        arrived(xb, rb, r, c)

        @pl.when(c < CUT)
        def _():
            go(kind, c, at(xb, r, c), xb, rb, r, dev)

        @pl.when((c >= CUT) & (v == 1))
        def _():
            go_tail = copy(tail_at(r, c), tail_at(r, c), send.at[kind], rb.at[r, c], dev)
            go_tail.start()

    def end_waits(n):
        for i in range(CHUNKS // UNITS):
            c = n * (CHUNKS // UNITS) + i
            for r in (own, sib):
                pl.when(jnp.logical_not(at_home | hop0 | hop1) & (c < CUT))(lambda: arrived(xb, rb, r, c))
            for r in (opp, dia):
                pl.when(jnp.logical_not(at_home | hop1) & ((c < CUT) | (u == 0)))(lambda: arrived(xb, rb, r, c))

    def stage_load(src):
        return pltpu.make_async_copy(src, stage, stage_sem.at[0])

    def band(ref, r):
        return ref.at[pl.ds(pl.multiple_of(r * rows, rows), rows)]

    def go_across(kind, c, src, dev):
        @pl.when(c < CUT)
        def _():
            go(kind, c, src, xb, rb, own, dev)

        @pl.when(c >= CUT)
        def _():
            copy(src, tail_at(opp, c), send.at[kind], rb.at[own, c], dev).start()

    def rest(ref, half):
        r = pl.ds(pl.multiple_of(half * 2 * rows, 2 * rows), 2 * rows)
        return rhs.at[0, r, pl.ds(0, TAIL * step)]

    lhs_save = pltpu.make_async_copy(lhs, lhs_out, lhs_sem.at[0])

    for i in range(occ.shape[0]):
        gap = virt[...] - occ[i]
        wt[:, pl.ds(i * virt.shape[1], virt.shape[1])] = 2.0 * gap / (gap * gap + freq[0] * freq[0])

    @pl.loop(0, TICKS)
    def _(t):
        m, phase = t // 3, lax.rem(t, 3)

        @pl.when((t + 2 < CHUNKS) & (t >= 0))
        def _():
            line_own(t + 2)

        @pl.when(t < CHUNKS)
        def _():
            arrived(xz, rz, opp, t)
            src = at(xz, opp, t)
            pl.when(lift & jnp.logical_not(aside(t)))(lambda: go_xb(UP_OPP, t, src, opp, up1))
            pl.when((v == 1) & (t < HELD))(lambda: go(DOWN_OPP, t, src, xb, rb, opp, down1))
            go(FWD, t, src, xz, rz, opp, to_sib)

            @pl.when((u == 0) & (v == 1))
            def _():
                hop(HOP_OWN, own, t, up0)
                hop(HOP_SIB, sib, t, up0)

        @pl.when((t >= 1) & (t < CHUNKS + 1))
        def _():
            arrived(xz, rz, dia, t - 1)

            @pl.when(lift & jnp.logical_not(aside(t - 1)))
            def _():
                go_xb(UP_DIA, t - 1, at(xz, dia, t - 1), dia, up1)

        held = HELD + t - (CHUNKS + 2)

        @pl.when((v == 1) & (held >= HELD) & (held < CUT))
        def _():
            go(DOWN, held, at(x, 0, held), xb, rb, own, down1)
            go(DOWN_OPP, held, at(xz, opp, held), xb, rb, opp, down1)

        slow, burst = m - 2, t - 2 * HELD
        late = jnp.where(v == 0, jnp.where(burst >= HELD - 3, burst, slow), t - 2 + v)
        paced = (v > 0) | ((phase == 1) & (slow < HELD - 3)) | (burst >= HELD - 3)

        @pl.when((v <= 2) & paced & (late >= 0) & (late < CHUNKS))
        def _():
            arrived(tr, rt, 0, late)
            src = at(tr, 0, late)
            pl.when(v >= 1)(lambda: go(PASS, late, src, tr, rt, 0, down_same))
            go_across(CROSS, late, src, across)

        @pl.when((v == 2) & (t == CHUNKS // 2))
        def _():
            @pl.loop(0, CHUNKS)
            def _(c):
                pl.when(aside(c))(lambda: go(SIDE, c, at(x, 0, c), ts, rs, 0, down_same))

        side = t - (CHUNKS + 2) + CUT - 7

        @pl.when((v == 1) & (t >= CHUNKS + 2) & aside(side))
        def _():
            arrived(ts, rs, 0, side)
            go(SIDE_CROSS, side, at(ts, 0, side), xb, rb, own, (2 - y, z))

        @pl.when(hop1)
        def _():
            @pl.when((phase == 0) & (m >= 2) & (m < CHUNKS + 2))
            def _():
                hop(HOP_DIA, dia, m - 2, up1)

            @pl.when(t < 2)
            def _():
                hop(HOP_OWN, own, t, up1)
                hop(HOP_SIB, sib, t, up1)

            @pl.when((phase == 1) & (m < CHUNKS - 2))
            def _():
                hop(HOP_OWN, own, m + 2, up1)

            @pl.when((phase == 2) & (m < CHUNKS - 2))
            def _():
                hop(HOP_SIB, sib, m + 2, up1)

            @pl.when((phase == 2) & (m < CHUNKS))
            def _():
                hop(HOP_OPP, opp, m, up1)

        @pl.when((u == 0) & (v == 2) & (m >= 1) & (m <= CHUNKS))
        def _():
            pl.when(phase == 0)(lambda: hop(HOP_OWN, own, m - 1, up0))
            pl.when(phase == 1)(lambda: hop(HOP_SIB, sib, m - 1, up0))

        @pl.when(t == 9)
        def _():
            @pl.loop(0, CHUNKS)
            def _(c):
                arrived(xz, rz, sib, c)

        @pl.when(at_home & (t == CHUNKS + 5))
        def _():
            near = rhs.at[0, :, pl.ds(0, TAIL * step)]
            load_columns(x, xz, xb, near, rhs_sem.at[0], at_home, own, CUT // TAIL, TAIL * step)
            await_columns(xb, near, rhs_sem.at[0], rows, TAIL * step)
            saves = [
                pltpu.make_async_copy(rest(tail_h, y), tail_h, tail_sem.at[0]),
                pltpu.make_async_copy(rest(tail_o, 1 - y), tail_o, tail_sem.at[1]),
            ]
            for save in saves:
                save.start()
            for save in saves:
                save.wait()

        fill = (t == 3) | (t == 10) | (t == CHUNKS + 1) | (t == CHUNKS + 2)

        @pl.when(fill)
        def _():
            r = jnp.where(t == 3, own, jnp.where(t == 10, sib, jnp.where(t == CHUNKS + 1, opp, dia)))
            stage_load(x).wait()
            scale = wt[:, pl.ds(pl.multiple_of(r * rows, rows), rows)]

            @pl.loop(0, TILES)
            def _(i):
                p = pl.ds(pl.multiple_of(i * tile, tile), tile)
                turned = stage[:, p].T.astype(jnp.float32) * scale
                lhs[p, pl.ds(pl.multiple_of(r * rows, rows), rows)] = turned.astype(jnp.bfloat16)

        pl.when(t == CHUNKS + 3)(lambda: lhs_save.start())
        pl.when(t == 1)(lambda: stage_load(x).start())
        pl.when(t == 9)(lambda: stage_load(band(xz, sib)).start())
        pl.when(t == CHUNKS)(lambda: stage_load(band(xz, opp)).start())
        pl.when(t == CHUNKS + 1)(lambda: stage_load(band(xz, dia)).start())

        work = t - FIRST
        n, q = work // SPAN, lax.rem(work, SPAN)

        @pl.when((work >= 0) & (work < SPAN * EARLY))
        def _():
            s = lax.rem(n, 2)

            @pl.when(q == 0)
            def _():
                await_columns(xb, rhs.at[s], rhs_sem.at[s], rows, width)

            for j in range(PER_TICK):
                p = PER_TICK * q + j
                got = jnp.dot(
                    lhs[pl.ds(pl.multiple_of(p * tile, tile), tile), :], rhs[s], preferred_element_type=jnp.float32
                )
                kept[
                    pl.ds(pl.multiple_of(p * tile, tile), tile), pl.ds(pl.multiple_of(n * width, width), width)
                ] = got.astype(jnp.bfloat16)

        ahead = work + 1
        n_ahead = ahead // SPAN

        @pl.when((ahead >= 0) & (ahead < SPAN * EARLY) & (lax.rem(ahead, SPAN) == 0))
        def _():
            end_waits(n_ahead)
            s = lax.rem(n_ahead, 2)
            load_columns(x, xz, xb, rhs.at[s], rhs_sem.at[s], at_home, own, n_ahead, width)

    def drain(kind, count):
        sent = x.at[:, pl.ds(0, count * step)]
        copy(sent, sent, send.at[kind], rz.at[0, 0], to_sib).wait_send()

    def drain_if(cond, kind, count):
        pl.when(cond)(lambda: drain(kind, count))

    def finals():
        @pl.loop(EARLY, UNITS)
        def _(n):
            end_waits(n)

    few = CUT - 1 - (CUT - 7)
    lhs_save.wait()
    for kind in (TO_SIB, TO_OPP, FWD):
        drain(kind, CHUNKS)
    drain_if(v == 2, SIDE, few)
    drain_if(v == 1, SIDE_CROSS, few)
    drain_if(v <= 2, CROSS, CHUNKS)
    drain_if((v == 1) | (v == 2), PASS, CHUNKS)
    drain_if(v == 0, UP, CHUNKS)
    drain_if(v == 3, DOWN, CHUNKS)
    finals()
    drain_if(v == 1, UP, CHUNKS)
    for kind in (UP_OPP, UP_DIA):
        drain_if(lift, kind, CHUNKS - few)
    for kind in (DOWN, DOWN_OPP):
        drain_if(v == 1, kind, CUT)
    for kind in (HOP_OWN, HOP_SIB):
        drain_if((u == 0) & (v == 1), kind, CHUNKS)
        drain_if(v == 2, kind, CUT)
    for kind in (HOP_OPP, HOP_DIA):
        drain_if(hop1, kind, CUT)


def gather(pair_block, occ_energy, virt_energy, frequency):
    rows, cols = pair_block.shape
    width, narrow = cols // UNITS, cols * TAIL // CHUNKS
    bf16 = jnp.bfloat16
    full = jax.ShapeDtypeStruct((4 * rows, cols), bf16)
    block = jax.ShapeDtypeStruct((rows, cols), bf16)
    half = jax.ShapeDtypeStruct((2 * rows, narrow), bf16)
    return pl.pallas_call(
        gather_kernel,
        out_shape=(
            full, full, block, block, half, half,
            jax.ShapeDtypeStruct((cols, 4 * rows), bf16),
            pltpu.VMEM((cols, 4 * rows), bf16),
            pltpu.VMEM((cols, EARLY * width), bf16),
        ),
        in_specs=[pl.BlockSpec(memory_space=m) for m in (pl.ANY, pltpu.SMEM, pltpu.VMEM, pltpu.SMEM)],
        out_specs=[pl.BlockSpec(memory_space=m) for m in (pltpu.HBM,) * 7 + (pltpu.VMEM,) * 2],
        scratch_shapes=[
            pltpu.VMEM((rows, cols), bf16),
            pltpu.VMEM((2, 4 * rows, width), bf16),
            pltpu.VMEM((1, 4 * rows), jnp.float32),
            pltpu.SemaphoreType.DMA((16,)),
            pltpu.SemaphoreType.DMA((4, CHUNKS)),
            pltpu.SemaphoreType.DMA((4, CHUNKS)),
            pltpu.SemaphoreType.DMA((1, CHUNKS)),
            pltpu.SemaphoreType.DMA((1, CHUNKS)),
            pltpu.SemaphoreType.DMA((1,)),
            pltpu.SemaphoreType.DMA((2, 4)),
            pltpu.SemaphoreType.DMA((2,)),
            pltpu.SemaphoreType.DMA((1,)),
        ],
        compiler_params=pltpu.CompilerParams(collective_id=0, has_side_effects=True, vmem_limit_bytes=13 * MIB),
    )(pair_block, occ_energy, virt_energy[None, :], frequency)


def span(i, size):
    return pl.ds(pl.multiple_of(i * size, size), size)


def finish_kernel(x, xz, xb, lhs, kept, out, rhs, acc, hold, rhs_sem, acc_sem, out_sem):
    rows, cols = x.shape
    width, tile, narrow = cols // UNITS, cols // TILES, cols * TAIL // CHUNKS
    strip = tile // STRIPS
    done = EARLY * width
    mid = cols - narrow - done
    b, z, y, k, u, v = place()

    def put(i):
        s = lax.rem(i, SLOTS)
        return pltpu.make_async_copy(hold.at[s], out.at[span(i, strip), pl.ds(0, done)], out_sem.at[s])

    def store(p):
        s = lax.rem(p, 2)
        cut = pl.ds(done, mid)
        return pltpu.make_async_copy(acc.at[s], out.at[span(p, tile), cut], acc_sem.at[s])

    load_columns(x, xz, xb, rhs, rhs_sem, u == v, b, EARLY, width, mid // width)

    @pl.loop(0, TILES)
    def _(p):
        for j in range(STRIPS):
            i = p * STRIPS + j
            pl.when(i >= SLOTS)(lambda: put(i - SLOTS).wait())
            hold[lax.rem(i, SLOTS)] = kept[span(i, strip), :].astype(jnp.float32)
            put(i).start()
        pl.when(p == 0)(lambda: await_columns(xb, rhs, rhs_sem, rows, mid))
        pl.when(p >= 2)(lambda: store(p - 2).wait())
        acc[lax.rem(p, 2)] = jnp.dot(lhs[span(p, tile), :], rhs[...], preferred_element_type=jnp.float32)
        store(p).start()

    for p in range(TILES - 2, TILES):
        store(p).wait()
    for i in range(TILES * STRIPS - SLOTS, TILES * STRIPS):
        put(i).wait()


def finish(pair_block, xz, xb, lhs, kept):
    rows, cols = pair_block.shape
    width, tile, narrow = cols // UNITS, cols // TILES, cols * TAIL // CHUNKS
    mid = cols - narrow - EARLY * width
    bf16, f32 = jnp.bfloat16, jnp.float32
    return pl.pallas_call(
        finish_kernel,
        out_shape=jax.ShapeDtypeStruct((cols, cols), f32),
        in_specs=[pl.BlockSpec(memory_space=m) for m in (pl.ANY,) * 3 + (pltpu.VMEM,) * 2],
        out_specs=pl.BlockSpec(memory_space=pl.ANY),
        scratch_shapes=[
            pltpu.VMEM((4 * rows, mid), bf16),
            pltpu.VMEM((2, tile, mid), f32),
            pltpu.VMEM((SLOTS, tile // STRIPS, EARLY * width), f32),
            pltpu.SemaphoreType.DMA((4,)),
            pltpu.SemaphoreType.DMA((2,)),
            pltpu.SemaphoreType.DMA((SLOTS,)),
        ],
        cost_estimate=pl.CostEstimate(flops=10**10, bytes_accessed=cols * cols * 4, transcendentals=0),
        compiler_params=pltpu.CompilerParams(vmem_limit_bytes=17 * MIB),
    )(pair_block, xz, xb, lhs, kept)


def tail_kernel(lhs_in, tail_h, tail_o, got_h, got_o, _, out, lhs, rhs, acc, lhs_sem, rhs_sem, acc_sem):
    cols = out.shape[0]
    tile, narrow = cols // TILES, rhs.shape[1]
    half = tail_h.shape[0]
    b, z, y, k, u, v = place()
    parts = [(tail_h, got_h, y, (v == 3) | ((v == 0) & (u == 1))), (tail_o, got_o, 1 - y, (u == 1) & ((v == 3) | (v == 0)))]

    def fetch(src, at, i):
        return pltpu.make_async_copy(src, rhs.at[pl.ds(pl.multiple_of(at * half, half), half)], rhs_sem.at[i])

    def store(p):
        s = lax.rem(p, 2)
        return pltpu.make_async_copy(acc.at[s], out.at[span(p, tile), pl.ds(cols - narrow, narrow)], acc_sem.at[s])

    def turn(p):
        return pltpu.make_async_copy(lhs_in.at[span(p, tile)], lhs.at[lax.rem(p, 3)], lhs_sem.at[lax.rem(p, 3)])

    turn(0).start()
    for i, (near, far, at, remote) in enumerate(parts):
        pl.when(remote)(lambda: fetch(far, at, i).start())
        pl.when(jnp.logical_not(remote))(lambda: fetch(near, at, i).start())
    turn(1).start()
    for i, (near, far, at, remote) in enumerate(parts):
        fetch(near, at, i).wait()

    @pl.loop(0, TILES)
    def _(p):
        turn(p).wait()
        pl.when(p + 2 < TILES)(lambda: turn(p + 2).start())
        pl.when(p >= 2)(lambda: store(p - 2).wait())
        acc[lax.rem(p, 2)] = jnp.dot(lhs[lax.rem(p, 3)], rhs[...], preferred_element_type=jnp.float32)
        store(p).start()

    for p in range(TILES - 2, TILES):
        store(p).wait()


def close(lhs, tail_h, tail_o, got_h, got_o, out):
    cols, depth = lhs.shape
    tile, narrow = cols // TILES, tail_h.shape[1]
    return pl.pallas_call(
        tail_kernel,
        out_shape=jax.ShapeDtypeStruct(out.shape, out.dtype),
        in_specs=[pl.BlockSpec(memory_space=m) for m in (pl.ANY,) * 6],
        out_specs=pl.BlockSpec(memory_space=pl.ANY),
        scratch_shapes=[
            pltpu.VMEM((3, tile, depth), jnp.bfloat16),
            pltpu.VMEM((depth, narrow), jnp.bfloat16),
            pltpu.VMEM((2, tile, narrow), jnp.float32),
            pltpu.SemaphoreType.DMA((3,)),
            pltpu.SemaphoreType.DMA((2,)),
            pltpu.SemaphoreType.DMA((2,)),
        ],
        input_output_aliases={5: 0},
        compiler_params=pltpu.CompilerParams(vmem_limit_bytes=49 * MIB),
    )(lhs, tail_h, tail_o, got_h, got_o, out)


def last_hops(groups):
    def index(g, b, z):
        return (g * 4 + b) * 4 + z

    both, lone = [], []
    for i in range(groups * 16):
        g, b, z = i // 16, i // 4 % 4, i % 4
        y, k = b // 2, b % 2
        u, v = k + y - 2 * y * k, z + y * (3 - 2 * z)
        d = 1 - 2 * y
        if v == 2:
            both.append((i, index(g, b, z + d)))
            if u == 1:
                lone.append((i, index(g, b, z + d)))
        if v == 1 and u == 1:
            both.append((i, index(g, b, z - d)))
            lone.append((i, index(g, b, z - d)))
    return both, lone


def shards(square, groups, pair_block, occ_energy, virt_energy, frequency):
    if square:
        xz, xb, _, _, tail_h, tail_o, lhs_back, lhs, kept = gather(pair_block, occ_energy, virt_energy, frequency)
        both, lone = last_hops(groups)
        axes = ("groups", "blk", "col")
        got_h = lax.ppermute(tail_h, axes, both)
        got_o = lax.ppermute(tail_o, axes, lone)
        lhs = pltpu.with_memory_space_constraint(lhs, pltpu.VMEM)
        kept = pltpu.with_memory_space_constraint(kept, pltpu.VMEM)
        out = finish(pair_block, xz, xb, lhs, kept)
        return close(lhs_back, tail_h, tail_o, got_h, got_o, out)
    weights = pair_weights(occ_energy, virt_energy, frequency)
    row_full = lax.all_gather(pair_block, "col", axis=1, tiled=True)
    column_slab = lax.all_to_all(row_full, "blk", split_axis=1, concat_axis=0, tiled=True)
    own_columns = lax.all_gather(pair_block, "blk", axis=0, tiled=True)
    scaled = (own_columns.astype(jnp.float32) * weights[:, None]).astype(jnp.bfloat16)
    return lax.dot_general(
        scaled, column_slab, (((0,), (0,)), ((), ())), preferred_element_type=jnp.float32
    )


def solution(mesh):
    square = mesh.shape["blk"] == 4 and mesh.shape["col"] == 4
    return jax.shard_map(
        functools.partial(shards, square, mesh.shape["groups"]),
        mesh=mesh,
        in_specs=(P(("groups", "blk"), "col"), P("groups"), P("groups"), P("groups")),
        out_specs=P(("groups", "col"), "blk"),
        check_vma=False,
    )
```
